32 devices in a mesh: dp: 2 (over x), expert: 16 (over z, y, core).
Axes of the slice: x: 2, y: 2, z: 4, core: 2. Of those that a mesh axis runs over, the one named last changes fastest.
Arguments:
- cotangent: bfloat16 [4096, 3584], P(('dp', 'expert')), may hold values from -0.59765625 to 0.59765625
- expert_ids: int32 [4096, 1], P(('dp', 'expert')), may hold values from 0 to 3; in each aligned block of 128 rows (0 to 127, 128 to 255, ...) at most 48 rows name the same one
- route_weights: float32 [4096, 1], P(('dp', 'expert')), may hold values from 0.1 to 1
- gate_pre: bfloat16 [1536, 4096], P('dp', 'expert'), may hold values from -5 to 5
- up_pre: bfloat16 [1536, 4096], P('dp', 'expert'), may hold values from -5 to 5
- down_weight: bfloat16 [3584, 4096], P('dp', 'expert'), may hold values from -0.1875 to 0.1875
Outputs:
- weight_grad: bfloat16 [3584, 4096], P('dp', 'expert')
- gate_grad: bfloat16 [1536, 4096], P('dp', 'expert')
- up_grad: bfloat16 [1536, 4096], P('dp', 'expert')
The draws below stay inside these ranges and needn't reach their ends.
Inputs may be any that keep to these rules, and one draw needn't show every extreme that they name: `expert_ids`: each token names one expert. Among the tokens of one device, at most 48 name the same expert, and in every draw some expert is named by exactly 48 tokens of some device.
All inputs are finite; a program needn't handle non-finite values.
Results may differ from the reference program's by a relative error of at most 0.013.
Values may be sent and summed in bfloat16 or wider, within the bound.
A program may use at most 64 MiB of HBM per device.

```python
import math
import jax
import jax.numpy as jnp
import numpy as np
from jax import lax

D = 3584
FFW = 1024
TOP = 1
TOK_DEV = 128
EXPERTS = 4
CAP = 48
TOKENS = 4096
SLOTS = 1536
N_DP = 2
N_EXPERT = 16


def shard_levels(own_key, extent, split, low, largest):
    def one(axis_at, parts):
        steps = jax.random.uniform(jax.random.fold_in(jax.random.fold_in(own_key, 6), axis_at), (parts,), jnp.float32, low / len(split), largest / len(split))
        return jnp.repeat(jnp.exp(steps), extent[axis_at] // parts).reshape((-1,) + (1,) * (len(extent) - axis_at - 1))

    gain = one(*split[0])
    for cut in split[1:]:
        gain = gain * one(*cut)
    return gain


def assign_block(own_key, own, number, rows, count, top, limit, skew):
    order = jax.random.permutation(own_key, count)
    heavy_load, common = load_shares(count, rows * top, limit, skew, True), load_shares(count, rows * top, limit, skew, False)
    places = jnp.arange(count)

    def named(lengths, turn):
        used = int((lengths > 0).sum())
        fixed = max(1, used // 4)
        shifted = fixed + (places - fixed + turn * (used - fixed)) % max(1, count - fixed)
        return jnp.zeros((count,), jnp.int32).at[order[jnp.where(places < fixed, places, shifted)]].set(jnp.asarray(lengths, jnp.int32))

    lengths = jnp.where(number % 4 == 0, named(heavy_load, number // 4), named(common, number - number // 4 - 1))
    mixed = jax.random.permutation(jax.random.fold_in(own, 3), count)
    source_of, receiver = mixed[0:count // 2 * 2:2], mixed[1:count // 2 * 2:2]
    room = jnp.minimum(lengths[source_of] - 1, limit - lengths[receiver]) // 2
    room = jnp.where((source_of == order[0]) | (receiver == order[0]) | (lengths[receiver] == 0), 0, jnp.maximum(room, 0))
    shifted = jax.random.randint(jax.random.fold_in(own, 4), (count // 2,), 0, 1 << 20) % (room + 1)
    lengths = lengths.at[source_of].add(-shifted).at[receiver].add(shifted)
    labels = jnp.searchsorted(jnp.cumsum(lengths), jnp.arange(rows * top), side="right").astype(jnp.int32)
    listing = labels.reshape(top, rows).T
    listing = listing[jax.random.permutation(jax.random.fold_in(own, 1), rows)]
    turn = jax.random.randint(jax.random.fold_in(own, 2), (rows, 1), 0, top)
    return jnp.take_along_axis(listing, (jnp.arange(top)[None, :] + turn) % top, axis=1)


def load_shares(count, total, most, lean, full):
    weights = [(1 << 20) // math.isqrt(standing ** lean) + 1 for standing in range(1, count + 1)]
    largest = most if full else min(most, max(-(-total // count), total * weights[0] // sum(weights)))
    least = 1 if total - largest >= count - 1 else 0
    holding, surplus = [largest] + [least] * (count - 1), total - largest - least * (count - 1)
    while surplus > 0:
        movable = [i for i in range(1, count) if holding[i] < largest] or [i for i in range(1, count) if holding[i] < most]
        whole, left = sum([weights[i] for i in movable]), surplus
        for i in movable:
            more = min(most - holding[i], max(1, left * weights[i] // whole), surplus)
            holding[i] = holding[i] + more
            surplus = surplus - more
    return np.array(holding)


def normal_values(rng, extent, width, limit, cuts=(), kind=jnp.bfloat16):
    drawn = width * jax.random.normal(rng, extent, jnp.float32)
    if cuts:
        drawn = drawn * shard_levels(rng, extent, cuts, -0.22, 0.18)
    return jnp.clip(drawn, -limit, limit).astype(kind)


def setup_inputs(seed: int = 0) -> dict:
    splits = jax.random.split(jax.random.key(seed), 7)
    cotangent = normal_values(splits[0], (TOKENS, D), 0.1, 0.59765625, ((0, 32),))
    expert_ids_keys = jax.random.split(jax.random.fold_in(splits[1], 1), TOKENS // TOK_DEV)
    expert_ids_turns = jax.random.permutation(jax.random.fold_in(splits[1], 3), TOKENS // TOK_DEV)
    expert_ids = jax.vmap(lambda own, number: assign_block(jax.random.fold_in(splits[1], 2), own, number, TOK_DEV, EXPERTS, TOP, CAP, 2))(expert_ids_keys, expert_ids_turns).reshape((TOKENS, TOP))
    route_weights = jnp.clip(0.1 + 0.9 * jax.random.uniform(splits[2], (TOKENS, TOP), jnp.float32) ** shard_levels(splits[2], (TOKENS, TOP), ((0, 32),), -0.2, 0.2), 0.1, 1.0)
    gate_pre = normal_values(splits[3], (SLOTS, EXPERTS * FFW), 1.0, 5.0, ((0, 2), (1, 16)))
    up_pre = normal_values(splits[4], (SLOTS, EXPERTS * FFW), 1.0, 5.0, ((0, 2), (1, 16)))
    down_weight = normal_values(splits[5], (D, EXPERTS * FFW), FFW ** -0.5, 0.1875, ((0, 2), (1, 16)))
    return {"cotangent": cotangent, "expert_ids": expert_ids, "route_weights": route_weights, "gate_pre": gate_pre, "up_pre": up_pre, "down_weight": down_weight}


def group_terms(cotangent, expert_ids, route_weights, gate_pre, up_pre, down_weight):
    onehot = (expert_ids[..., None] == jnp.arange(EXPERTS, dtype=jnp.int32)).astype(jnp.int32)
    touched = jnp.sum(onehot, axis=2)
    earlier = jnp.cumsum(touched, axis=1) - touched
    position = jnp.sum(onehot * earlier[:, :, None, :], axis=3)
    sources = jnp.arange(N_EXPERT, dtype=jnp.int32)[:, None, None] * CAP
    rows = (sources + position).astype(jnp.int32)
    scaled = route_weights[..., None] * cotangent.astype(jnp.float32)[:, :, None, :]
    routed = jnp.zeros((EXPERTS, N_EXPERT * CAP, D), jnp.float32).at[expert_ids, rows].add(scaled)
    routed_half = lax.optimization_barrier(routed.astype(jnp.bfloat16))
    routed_full = routed_half.astype(jnp.float32)
    weights = down_weight.astype(jnp.float32).reshape(D, EXPERTS, FFW)
    gate_full = gate_pre.astype(jnp.float32).reshape(N_EXPERT * CAP, EXPERTS, FFW)
    up_full = up_pre.astype(jnp.float32).reshape(N_EXPERT * CAP, EXPERTS, FFW)
    upstream = jnp.einsum('xrd,dxf->rxf', routed_full, weights)
    sigmoid = jax.nn.sigmoid(gate_full)
    active = gate_full * sigmoid
    product_half = lax.optimization_barrier((active * up_full).astype(jnp.bfloat16))
    gate_grad = (upstream * up_full * sigmoid * (1.0 + gate_full * (1.0 - sigmoid))).astype(jnp.bfloat16)
    up_grad = (upstream * active).astype(jnp.bfloat16)
    partial_sum = jnp.einsum('xrd,rxf->dxf', routed_full, product_half.astype(jnp.float32))
    partial_half = partial_sum.reshape(D, EXPERTS * FFW).astype(jnp.bfloat16)
    return partial_half, gate_grad.reshape(N_EXPERT * CAP, EXPERTS * FFW), up_grad.reshape(N_EXPERT * CAP, EXPERTS * FFW)


def reference(cotangent, expert_ids, route_weights, gate_pre, up_pre, down_weight):
    stacked = (cotangent.reshape(N_DP, N_EXPERT, TOK_DEV, D),
               expert_ids.reshape(N_DP, N_EXPERT, TOK_DEV, TOP),
               route_weights.reshape(N_DP, N_EXPERT, TOK_DEV, TOP),
               gate_pre.reshape(N_DP, N_EXPERT * CAP, EXPERTS * FFW),
               up_pre.reshape(N_DP, N_EXPERT * CAP, EXPERTS * FFW))

    def step(total, pieces):
        partial_half, gate_grad, up_grad = group_terms(pieces[0], pieces[1], pieces[2], pieces[3], pieces[4], down_weight)
        return total + partial_half.astype(jnp.float32), (gate_grad, up_grad)

    start = jnp.zeros((D, EXPERTS * FFW), jnp.float32)
    total, grads = lax.scan(step, start, stacked)
    weight_grad = total.astype(jnp.bfloat16)
    gate_grad = grads[0].reshape(SLOTS, EXPERTS * FFW)
    up_grad = grads[1].reshape(SLOTS, EXPERTS * FFW)
    return weight_grad, gate_grad, up_grad
```

```python
import functools

import jax
import jax.numpy as jnp
from jax import lax
from jax.experimental import pallas as pl
from jax.experimental.pallas import tpu as pltpu
from jax.sharding import PartitionSpec as P

SPLIT = 4


def kernel(
    sizes,
    cot_ref,
    ids_ref,
    weights_ref,
    gate_ref,
    up_ref,
    down_ref,
    wgrad_ref,
    ggrad_ref,
    ugrad_ref,
    sendbuf,
    routed,
    down_in,
    part_out,
    part_in,
    upstream,
    slope,
    active,
    product,
    picker,
    scale,
    z_send,
    z_recv,
    y_send,
    y_recv,
    c_send,
    c_recv,
    w_send,
    w_recv,
    g_send,
    g_recv,
):
    n, experts, cap, chunks, width, aligned = sizes
    own = chunks // n
    away = chunks - own
    tokens = ids_ref.shape[0]
    dp = lax.axis_index("dp")
    me = lax.axis_index("expert")
    e, lane = me // SPLIT, me % SPLIT
    across = me - lane + (lane + 2) % SPLIT
    beside = me - lane + (lane // 2) * 2 + (lane + 1) % 2
    lane_across = (lane + 2) % SPLIT

    barrier = pltpu.get_barrier_semaphore()

    def greet(target):
        pl.semaphore_signal(
            barrier, inc=1, device_id=target, device_id_type=pl.DeviceIdType.MESH
        )

    for k in range(1, experts):
        greet({"expert": (e + k) % experts * SPLIT + lane})
    greet({"expert": across})
    greet({"expert": beside})
    for k in range(1, n):
        greet({"dp": (dp + k) % n})

    shape = (tokens, tokens)
    first, second = lax.broadcasted_iota(jnp.int32, shape, 0), lax.broadcasted_iota(jnp.int32, shape, 1)
    diagonal = first == second
    ids_row = jnp.sum(jnp.where(diagonal, ids_ref[...], 0), axis=0, keepdims=True)
    weight_row = jnp.sum(jnp.where(diagonal, weights_ref[...], 0.0), axis=0, keepdims=True)
    names = lax.broadcasted_iota(jnp.int32, (-(-experts // 16) * 16, tokens), 0) == ids_row
    before = jnp.where(first < second, 1.0, 0.0).astype(jnp.bfloat16)
    earlier = jnp.dot(
        jnp.where(names, 1.0, 0.0).astype(jnp.bfloat16), before, preferred_element_type=jnp.float32
    )
    position = jnp.sum(jnp.where(names, earlier, 0.0), axis=0, keepdims=True).astype(jnp.int32)
    target = ids_row * cap + position
    chosen = lax.broadcasted_iota(jnp.int32, (experts * cap, tokens), 0) == target
    picker[...] = jnp.where(chosen, 1.0, 0.0).astype(jnp.bfloat16)
    scale[...] = jnp.sum(jnp.where(chosen, weight_row, 0.0), axis=1, keepdims=True)

    def block_of(q):
        return (dp + 1 + q // own) % n * own + q % own

    def build(q):
        if aligned:
            columns = cot_ref[:, pl.ds(pl.multiple_of(block_of(q) * width, 128), width)]
        else:
            columns = cot_ref[block_of(q)]
        picked = jnp.dot(picker[...], columns, preferred_element_type=jnp.float32)
        rows = (picked * scale[...]).astype(jnp.bfloat16).reshape(experts, cap, width)
        sendbuf[q] = rows
        routed[q, e, lane] = sendbuf[q, e]

    def to_expert(q):
        for k in range(1, experts):
            there = (e + k) % experts
            pltpu.make_async_remote_copy(
                src_ref=sendbuf.at[q, there],
                dst_ref=routed.at[q, e, lane],
                send_sem=z_send.at[q],
                recv_sem=z_recv.at[q],
                device_id={"expert": there * SPLIT + lane},
                device_id_type=pl.DeviceIdType.MESH,
            ).start()

    def relay(q, which, to, send, recv):
        return pltpu.make_async_remote_copy(
            src_ref=routed.at[q, :, which],
            dst_ref=routed.at[q, :, which],
            send_sem=send,
            recv_sem=recv,
            device_id={"expert": to},
            device_id_type=pl.DeviceIdType.MESH,
        )

    def over_y(q):
        return relay(q, lane, across, y_send.at[q], y_recv.at[q])

    def over_core(q, turn):
        which = lane if turn == 0 else lane_across
        return relay(q, which, beside, c_send.at[q, turn], c_recv.at[q, turn])

    def down_copy(q):
        piece = q % own
        return pltpu.make_async_remote_copy(
            src_ref=down_ref.at[piece],
            dst_ref=down_in.at[q],
            send_sem=w_send.at[q],
            recv_sem=w_recv.at[q],
            device_id={"dp": (dp - 1 - q // own + n) % n},
            device_id_type=pl.DeviceIdType.MESH,
        )

    def part_copy(q):
        return pltpu.make_async_remote_copy(
            src_ref=part_out.at[q],
            dst_ref=part_in.at[q],
            send_sem=g_send.at[q],
            recv_sem=g_recv.at[q],
            device_id={"dp": (dp + 1 + q // own) % n},
            device_id_type=pl.DeviceIdType.MESH,
        )

    build(0)
    pl.semaphore_wait(barrier, experts - 1 + 2 + n - 1)

    @pl.loop(0, away)
    def _(q):
        down_copy(q).start()

    @pl.loop(1, chunks)
    def _(q):
        build(q)
        to_expert(q - 1)

    to_expert(chunks - 1)

    rows_all = gate_ref.shape[0]
    piece = rows_all // 8

    @pl.loop(0, 8)
    def _(i):
        at = pl.ds(pl.multiple_of(i * piece, 16), piece)
        gate = gate_ref[at, :].astype(jnp.float32)
        up = up_ref[at, :].astype(jnp.float32)
        sig = jax.nn.sigmoid(gate)
        act = gate * sig
        active[at, :] = act
        slope[at, :] = up * sig * (1.0 + gate * (1.0 - sig))
        product[at, :] = (act * up).astype(jnp.bfloat16)
        upstream[at, :] = jnp.zeros_like(act)

    def all_but_one(ref_at, sem):
        pltpu.make_async_copy(ref_at, ref_at, sem).wait()

    def partial_of(q):
        rows = routed[q].reshape(rows_all, width)
        return rows, lax.dot_general(
            rows, product[...], (((0,), (0,)), ((), ())), preferred_element_type=jnp.float32
        ).astype(jnp.bfloat16)

    @pl.loop(0, chunks + 2)
    def _(t):
        @pl.when(t < chunks)
        def _():
            all_but_one(routed.at[t, pl.ds(0, experts - 1), 0], z_recv.at[t])
            over_y(t).start()
            over_core(t, 0).start()

        @pl.when((t >= 1) & (t < chunks + 1))
        def _():
            over_y(t - 1).wait_recv()
            over_core(t - 1, 1).start()

        @pl.when(t >= 2)
        def _():
            q = t - 2
            over_core(q, 0).wait_recv()
            over_core(q, 1).wait_recv()

            @pl.when(q < away)
            def _():
                rows, part = partial_of(q)
                part_out[q] = part
                down_copy(q).wait_recv()
                upstream[...] += jnp.dot(rows, down_in[q], preferred_element_type=jnp.float32)
                part_copy(q).start()

            @pl.when(q >= away)
            def _():
                j = q - away
                rows, part = partial_of(q)
                upstream[...] += jnp.dot(rows, down_ref[j], preferred_element_type=jnp.float32)
                total = part.astype(jnp.float32)
                for k in range(n - 1):
                    part_copy(k * own + j).wait_recv()
                    total = total + part_in[k * own + j].astype(jnp.float32)
                wgrad_ref[j] = total.astype(jnp.bfloat16)

    @pl.loop(0, 8)
    def _(i):
        at = pl.ds(pl.multiple_of(i * piece, 16), piece)
        ggrad_ref[at, :] = (upstream[at, :] * slope[at, :]).astype(jnp.bfloat16)
        ugrad_ref[at, :] = (upstream[at, :] * active[at, :]).astype(jnp.bfloat16)

    @pl.loop(0, chunks)
    def _(q):
        all_but_one(sendbuf.at[q, pl.ds(0, experts - 1)], z_send.at[q])
        over_y(q).wait_send()
        over_core(q, 0).wait_send()
        over_core(q, 1).wait_send()

    @pl.loop(0, away)
    def _(q):
        down_copy(q).wait_send()
        part_copy(q).wait_send()


def chunk_width(depth):
    for width in (256, 128):
        if depth % width == 0:
            return width, True
    return depth, False


def per_device(cotangent, expert_ids, route_weights, gate_pre, up_pre, down_weight):
    n = lax.axis_size("dp")
    devices = lax.axis_size("expert")
    experts = devices // SPLIT
    rows, hidden = gate_pre.shape
    capacity = rows // devices
    cap = -(-capacity // 16) * 16
    depth = down_weight.shape[0]
    width, aligned = chunk_width(depth)
    own = depth // width
    chunks = n * own
    away = chunks - own
    if not aligned:
        cotangent = cotangent.reshape(-1, chunks, width).swapaxes(0, 1)

    def widen(a):
        if cap == capacity:
            return a
        a = a.reshape(devices, capacity, hidden)
        return jnp.pad(a, ((0, 0), (0, cap - capacity), (0, 0))).reshape(devices * cap, hidden)

    def narrow(a):
        if cap == capacity:
            return a
        return a.reshape(devices, cap, hidden)[:, :capacity].reshape(rows, hidden)

    padded = devices * cap
    half, full = jnp.bfloat16, jnp.float32
    vmem = pl.BlockSpec(memory_space=pltpu.VMEM)
    dma = pltpu.SemaphoreType.DMA
    weight_grad, gate_grad, up_grad = pl.pallas_call(
        functools.partial(kernel, (n, experts, cap, chunks, width, aligned)),
        out_shape=(
            jax.ShapeDtypeStruct((own, width, hidden), half),
            jax.ShapeDtypeStruct((padded, hidden), half),
            jax.ShapeDtypeStruct((padded, hidden), half),
        ),
        in_specs=[vmem] * 6,
        out_specs=(vmem, vmem, vmem),
        scratch_shapes=[
            pltpu.VMEM((chunks, experts, cap, width), half),
            pltpu.VMEM((chunks, experts, SPLIT, cap, width), half),
            pltpu.VMEM((away, width, hidden), half),
            pltpu.VMEM((away, width, hidden), half),
            pltpu.VMEM((away, width, hidden), half),
            pltpu.VMEM((padded, hidden), full),
            pltpu.VMEM((padded, hidden), full),
            pltpu.VMEM((padded, hidden), full),
            pltpu.VMEM((padded, hidden), half),
            pltpu.VMEM((experts * cap, cotangent.shape[0] if aligned else cotangent.shape[1]), half),
            pltpu.VMEM((experts * cap, 1), full),
            dma((chunks,)),
            dma((chunks,)),
            dma((chunks,)),
            dma((chunks,)),
            dma((chunks, 2)),
            dma((chunks, 2)),
            dma((away,)),
            dma((away,)),
            dma((away,)),
            dma((away,)),
        ],
        compiler_params=pltpu.CompilerParams(collective_id=0, has_side_effects=True),
    )(
        cotangent,
        expert_ids,
        route_weights,
        widen(gate_pre),
        widen(up_pre),
        down_weight.reshape(own, width, hidden),
    )
    return weight_grad.reshape(depth, hidden), narrow(gate_grad), narrow(up_grad)


def solution(mesh):
    placed = (
        P(("dp", "expert"), None),
        P(("dp", "expert"), None),
        P(("dp", "expert"), None),
        P("dp", "expert"),
        P("dp", "expert"),
        P("dp", "expert"),
    )
    return jax.shard_map(
        per_device,
        mesh=mesh,
        in_specs=placed,
        out_specs=(P("dp", "expert"), P("dp", "expert"), P("dp", "expert")),
        check_vma=False,
    )
```

```python
import functools

import jax
import jax.numpy as jnp
from jax import lax
from jax.experimental import pallas as pl
from jax.experimental.pallas import tpu as pltpu
from jax.sharding import PartitionSpec as P

SPLIT = 4
EARLY = 2
BUILD = 3
LAG = 3


def kernel(
    sizes,
    cot_hbm,
    ids_ref,
    weights_ref,
    gate_hbm,
    up_hbm,
    down_hbm,
    wgrad_ref,
    ggrad_ref,
    ugrad_ref,
    cot_ref,
    gate_ref,
    up_ref,
    down_ref,
    load,
    sendbuf,
    routed,
    cot_in,
    ids_in,
    weights_in,
    up_out,
    up_in,
    upstream,
    slope,
    active,
    product,
    picker,
    scale,
    z_send,
    z_recv,
    y_send,
    y_recv,
    c_send,
    c_recv,
    x_send,
    x_recv,
    i_send,
    i_recv,
    p_send,
    p_recv,
    u_send,
    u_recv,
):
    n, experts, cap, chunks, width, aligned = sizes
    own = chunks // n
    away = chunks - own
    early = min(EARLY, own - 1)
    ahead = min(BUILD, chunks)
    tokens = ids_ref.shape[1]
    dp = lax.axis_index("dp")
    me = lax.axis_index("expert")
    e, lane = me // SPLIT, me % SPLIT
    across = me - lane + (lane + 2) % SPLIT
    beside = me - lane + (lane // 2) * 2 + (lane + 1) % 2
    lane_across = (lane + 2) % SPLIT

    loads = [
        pltpu.make_async_copy(source, to, load.at[i])
        for i, (source, to) in enumerate(
            ((cot_hbm, cot_ref), (gate_hbm, gate_ref), (up_hbm, up_ref), (down_hbm, down_ref))
        )
    ]
    for copy in loads:
        copy.start()

    barrier = pltpu.get_barrier_semaphore()

    def greet(target):
        pl.semaphore_signal(
            barrier, inc=1, device_id=target, device_id_type=pl.DeviceIdType.MESH
        )

    for k in range(1, experts):
        greet({"expert": (e + k) % experts * SPLIT + lane})
    greet({"expert": across})
    greet({"expert": beside})
    for k in range(1, n):
        greet({"dp": (dp + k) % n})

    def send(source, to, sent, arrived, device):
        return pltpu.make_async_remote_copy(
            src_ref=source,
            dst_ref=to,
            send_sem=sent,
            recv_sem=arrived,
            device_id=device,
            device_id_type=pl.DeviceIdType.MESH,
        )

    def chunk_at(t):
        late = jnp.where(t < early + away, own - early, -away)
        return t + jnp.where(t < early, 0, late)

    def columns_of(share, j):
        if aligned:
            return cot_ref.at[:, pl.ds(pl.multiple_of((share * own + j) * width, 128), width)]
        return cot_ref.at[share * own + j]

    def cot_copy(i):
        to = (dp - 1 - i // own + n) % n
        return send(columns_of(to, i % own), cot_in.at[i], x_send.at[i], x_recv.at[i], {"dp": to})

    def ids_copy(k):
        return send(
            ids_ref, ids_in.at[k - 1], i_send.at[k - 1, 0], i_recv.at[k - 1, 0], {"dp": (dp - k + n) % n}
        )

    def weights_copy(k):
        return send(
            weights_ref, weights_in.at[k - 1], i_send.at[k - 1, 1], i_recv.at[k - 1, 1], {"dp": (dp - k + n) % n}
        )

    def product_copy(k):
        return send(
            product.at[0], product.at[k], p_send.at[k - 1], p_recv.at[k - 1], {"dp": (dp - k + n) % n}
        )

    def up_copy(i):
        return send(up_out.at[i], up_in.at[i], u_send.at[i], u_recv.at[i], {"dp": (dp + 1 + i) % n})

    def pick(k, ids_row, weight_row):
        shape = (tokens, tokens)
        first = lax.broadcasted_iota(jnp.int32, shape, 0)
        second = lax.broadcasted_iota(jnp.int32, shape, 1)
        names = lax.broadcasted_iota(jnp.int32, (-(-experts // 16) * 16, tokens), 0) == ids_row
        before = jnp.where(first < second, 1.0, 0.0).astype(jnp.bfloat16)
        earlier = jnp.dot(
            jnp.where(names, 1.0, 0.0).astype(jnp.bfloat16), before, preferred_element_type=jnp.float32
        )
        position = jnp.sum(jnp.where(names, earlier, 0.0), axis=0, keepdims=True).astype(jnp.int32)
        target = ids_row * cap + position
        chosen = lax.broadcasted_iota(jnp.int32, (experts * cap, tokens), 0) == target
        picker[k] = jnp.where(chosen, 1.0, 0.0).astype(jnp.bfloat16)
        scale[k] = jnp.sum(jnp.where(chosen, weight_row, 0.0), axis=1, keepdims=True)

    def place(q, k, columns):
        picked = jnp.dot(picker[k], columns, preferred_element_type=jnp.float32)
        rows = (picked * scale[k]).astype(jnp.bfloat16).reshape(experts, cap, width)
        sendbuf[q] = rows
        routed[q, e, lane] = sendbuf[q, e]

    def build(t):
        q = chunk_at(t)

        @pl.when(q < own)
        def _():
            place(q, 0, columns_of(dp, q)[...])

        @pl.when(q >= own)
        def _():
            cot_copy(q - own).wait_recv()
            place(q, q // own, cot_in[q - own])

    def from_source(q, source):
        at = routed.at[q, source, lane]
        return send(at, at, y_send.at[q], y_recv.at[q], {"expert": across})

    def to_expert(t):
        q = chunk_at(t)
        for k in range(1, experts):
            there = (e + k) % experts
            send(
                sendbuf.at[q, there],
                routed.at[q, e, lane],
                z_send.at[q],
                z_recv.at[q],
                {"expert": there * SPLIT + lane},
            ).start()
        from_source(q, e).start()

    def over_y(q):
        at = routed.at[q, :, lane]
        return send(at, at, y_send.at[q], y_recv.at[q], {"expert": across})

    def over_core(q, turn):
        at = routed.at[q, :, lane if turn == 0 else lane_across]
        return send(at, at, c_send.at[q, turn], c_recv.at[q, turn], {"expert": beside})

    def all_but_one(ref_at, sem):
        pltpu.make_async_copy(ref_at, ref_at, sem).wait()

    pick(0, ids_ref[...], weights_ref[...])
    loads[0].wait()
    for j in range(early):
        place(j, 0, columns_of(dp, j)[...])
    pl.semaphore_wait(barrier, experts - 1 + 2 + n - 1)
    for k in range(1, n):
        ids_copy(k).start()
        weights_copy(k).start()

    @pl.loop(0, away)
    def _(i):
        cot_copy(i).start()

    for j in range(early):
        to_expert(j)

    rows_all = gate_ref.shape[0]
    piece = rows_all // 8
    loads[1].wait()
    loads[2].wait()

    @pl.loop(0, 8)
    def _(i):
        at = pl.ds(pl.multiple_of(i * piece, 16), piece)
        gate = gate_ref[at, :].astype(jnp.float32)
        up = up_ref[at, :].astype(jnp.float32)
        sig = jax.nn.sigmoid(gate)
        act = gate * sig
        active[at, :] = act
        slope[at, :] = up * sig * (1.0 + gate * (1.0 - sig))
        product[0, at, :] = (act * up).astype(jnp.bfloat16)
        for k in range(n):
            upstream[k, at, :] = jnp.zeros_like(act)

    for k in range(1, n):
        ids_copy(k).wait_recv()
        weights_copy(k).wait_recv()
        pick(k, ids_in[k - 1], weights_in[k - 1])
    for t in range(early, ahead):
        build(t)
    for t in range(early, ahead - 1):
        to_expert(t)
    for k in range(1, n):
        product_copy(k).start()
    loads[3].wait()

    def gradient(j):
        total = jnp.zeros((width, product.shape[2]), jnp.float32)
        for k in range(n):
            rows = routed[k * own + j].reshape(rows_all, width)
            total = total + lax.dot_general(
                rows, product[k], (((0,), (0,)), ((), ())), preferred_element_type=jnp.float32
            )
        wgrad_ref[j] = total.astype(jnp.bfloat16)

    @pl.loop(0, chunks + LAG + 1)
    def _(t):
        @pl.when(t + ahead < chunks)
        def _():
            build(t + ahead)

        @pl.when(t + ahead - 1 < chunks)
        def _():
            to_expert(t + ahead - 1)

        @pl.when(t < chunks)
        def _():
            q = chunk_at(t)
            all_but_one(routed.at[q, pl.ds(0, experts - 1), 0], z_recv.at[q])
            for k in range(1, experts):
                from_source(q, (e + k) % experts).start()
            over_core(q, 0).start()

        @pl.when((t >= LAG) & (t < chunks + LAG))
        def _():
            q = chunk_at(t - LAG)
            over_y(q).wait_recv()
            over_core(q, 1).start()

        @pl.when(t >= LAG + 1)
        def _():
            turn = t - LAG - 1
            q = chunk_at(turn)
            k, j = q // own, q % own
            over_core(q, 0).wait_recv()
            over_core(q, 1).wait_recv()
            rows = routed[q].reshape(rows_all, width)
            upstream[k] += jnp.dot(rows, down_ref[j], preferred_element_type=jnp.float32)

            @pl.when((k >= 1) & (j == own - 1))
            def _():
                up_out[k - 1] = upstream[k].astype(jnp.bfloat16)

            @pl.when(turn == early + away)
            def _():
                for i in range(1, n):
                    product_copy(i).wait_recv()
                for i in range(early):
                    gradient(i)

            @pl.when(turn >= early + away)
            def _():
                gradient(j)

            @pl.when((k >= 1) & (j == own - 1))
            def _():
                up_copy(k - 1).start()

    for k in range(1, n):
        up_copy(k - 1).wait_recv()

    @pl.loop(0, 8)
    def _(i):
        at = pl.ds(pl.multiple_of(i * piece, 16), piece)
        total = upstream[0, at, :]
        for k in range(1, n):
            total = total + up_in[k - 1, at, :].astype(jnp.float32)
        ggrad_ref[at, :] = (total * slope[at, :]).astype(jnp.bfloat16)
        ugrad_ref[at, :] = (total * active[at, :]).astype(jnp.bfloat16)

    @pl.loop(0, chunks)
    def _(q):
        all_but_one(sendbuf.at[q, pl.ds(0, experts - 1)], z_send.at[q])
        over_y(q).wait_send()
        over_core(q, 0).wait_send()
        over_core(q, 1).wait_send()

    @pl.loop(0, away)
    def _(i):
        cot_copy(i).wait_send()

    for k in range(1, n):
        ids_copy(k).wait_send()
        weights_copy(k).wait_send()
        product_copy(k).wait_send()
        up_copy(k - 1).wait_send()


def chunk_width(depth):
    for width in (256, 128):
        if depth % width == 0:
            return width, True
    return depth, False


def per_device(cotangent, expert_ids, route_weights, gate_pre, up_pre, down_weight):
    n = lax.axis_size("dp")
    devices = lax.axis_size("expert")
    experts = devices // SPLIT
    rows, hidden = gate_pre.shape
    capacity = rows // devices
    cap = -(-capacity // 16) * 16
    depth = down_weight.shape[0]
    width, aligned = chunk_width(depth)
    own = depth // width
    chunks = n * own
    away = chunks - own
    if not aligned:
        cotangent = cotangent.reshape(-1, chunks, width).swapaxes(0, 1)

    def widen(a):
        if cap == capacity:
            return a
        a = a.reshape(devices, capacity, hidden)
        return jnp.pad(a, ((0, 0), (0, cap - capacity), (0, 0))).reshape(devices * cap, hidden)

    def narrow(a):
        if cap == capacity:
            return a
        return a.reshape(devices, cap, hidden)[:, :capacity].reshape(rows, hidden)

    padded = devices * cap
    tokens = expert_ids.shape[0]
    half, full = jnp.bfloat16, jnp.float32
    vmem = pl.BlockSpec(memory_space=pltpu.VMEM)
    anywhere = pl.BlockSpec(memory_space=pl.ANY)
    dma = pltpu.SemaphoreType.DMA
    weight_grad, gate_grad, up_grad = pl.pallas_call(
        functools.partial(kernel, (n, experts, cap, chunks, width, aligned)),
        out_shape=(
            jax.ShapeDtypeStruct((own, width, hidden), half),
            jax.ShapeDtypeStruct((padded, hidden), half),
            jax.ShapeDtypeStruct((padded, hidden), half),
        ),
        in_specs=[anywhere, vmem, vmem, anywhere, anywhere, anywhere],
        out_specs=(vmem, vmem, vmem),
        scratch_shapes=[
            pltpu.VMEM(cotangent.shape, half),
            pltpu.VMEM((padded, hidden), half),
            pltpu.VMEM((padded, hidden), half),
            pltpu.VMEM((own, width, hidden), half),
            dma((4,)),
            pltpu.VMEM((chunks, experts, cap, width), half),
            pltpu.VMEM((chunks, experts, SPLIT, cap, width), half),
            pltpu.VMEM((away, tokens, width), half),
            pltpu.VMEM((n - 1, 1, tokens), jnp.int32),
            pltpu.VMEM((n - 1, 1, tokens), full),
            pltpu.VMEM((n - 1, padded, hidden), half),
            pltpu.VMEM((n - 1, padded, hidden), half),
            pltpu.VMEM((n, padded, hidden), full),
            pltpu.VMEM((padded, hidden), full),
            pltpu.VMEM((padded, hidden), full),
            pltpu.VMEM((n, padded, hidden), half),
            pltpu.VMEM((n, experts * cap, tokens), half),
            pltpu.VMEM((n, experts * cap, 1), full),
            dma((chunks,)),
            dma((chunks,)),
            dma((chunks,)),
            dma((chunks,)),
            dma((chunks, 2)),
            dma((chunks, 2)),
            dma((away,)),
            dma((away,)),
            dma((n - 1, 2)),
            dma((n - 1, 2)),
            dma((n - 1,)),
            dma((n - 1,)),
            dma((n - 1,)),
            dma((n - 1,)),
        ],
        compiler_params=pltpu.CompilerParams(collective_id=0, has_side_effects=True),
    )(
        cotangent,
        expert_ids.reshape(1, -1),
        route_weights.reshape(1, -1),
        widen(gate_pre),
        widen(up_pre),
        down_weight.reshape(own, width, hidden),
    )
    return weight_grad.reshape(depth, hidden), narrow(gate_grad), narrow(up_grad)


def solution(mesh):
    placed = (
        P(("dp", "expert"), None),
        P(("dp", "expert"), None),
        P(("dp", "expert"), None),
        P("dp", "expert"),
        P("dp", "expert"),
        P("dp", "expert"),
    )
    return jax.shard_map(
        per_device,
        mesh=mesh,
        in_specs=placed,
        out_specs=(P("dp", "expert"), P("dp", "expert"), P("dp", "expert")),
        check_vma=False,
    )
```

```python
import functools

import jax
import jax.numpy as jnp
from jax import lax
from jax.experimental import pallas as pl
from jax.experimental.pallas import tpu as pltpu
from jax.sharding import PartitionSpec as P

SPLIT = 4
EARLY = 2
BUILD = 3
LAG = 3


def kernel(
    sizes,
    cot_hbm,
    ids_hbm,
    weights_hbm,
    gate_hbm,
    up_hbm,
    down_hbm,
    wgrad_ref,
    ggrad_ref,
    ugrad_ref,
    cot_ref,
    ids_ref,
    weights_ref,
    gate_ref,
    up_ref,
    down_ref,
    load,
    sendbuf,
    routed,
    cot_in,
    ids_in,
    weights_in,
    up_out,
    up_in,
    upstream,
    slope,
    active,
    product,
    picker,
    scale,
    z_send,
    z_recv,
    y_send,
    y_recv,
    c_send,
    c_recv,
    x_send,
    x_recv,
    i_send,
    i_recv,
    p_send,
    p_recv,
    u_send,
    u_recv,
):
    n, experts, cap, chunks, width, aligned = sizes
    own = chunks // n
    away = chunks - own
    early = min(EARLY, own - 1)
    ahead = min(BUILD, chunks)
    tokens = ids_ref.shape[1]
    dp = lax.axis_index("dp")
    me = lax.axis_index("expert")
    e, lane = me // SPLIT, me % SPLIT
    across = me - lane + (lane + 2) % SPLIT
    beside = me - lane + (lane // 2) * 2 + (lane + 1) % 2
    lane_across = (lane + 2) % SPLIT

    loads = [
        pltpu.make_async_copy(source, to, load.at[i])
        for i, (source, to) in enumerate(
            (
                (cot_hbm, cot_ref),
                (gate_hbm, gate_ref),
                (up_hbm, up_ref),
                (down_hbm, down_ref),
                (ids_hbm, ids_ref),
                (weights_hbm, weights_ref),
            )
        )
    ]
    for i in (4, 5, 0, 1, 2, 3):
        loads[i].start()

    barrier = pltpu.get_barrier_semaphore()

    def greet(target):
        pl.semaphore_signal(
            barrier, inc=1, device_id=target, device_id_type=pl.DeviceIdType.MESH
        )

    for k in range(1, experts):
        greet({"expert": (e + k) % experts * SPLIT + lane})
    greet({"expert": across})
    greet({"expert": beside})
    for k in range(1, n):
        greet({"dp": (dp + k) % n})

    def send(source, to, sent, arrived, device):
        return pltpu.make_async_remote_copy(
            src_ref=source,
            dst_ref=to,
            send_sem=sent,
            recv_sem=arrived,
            device_id=device,
            device_id_type=pl.DeviceIdType.MESH,
        )

    def chunk_at(t):
        late = jnp.where(t < early + away, own - early, -away)
        return t + jnp.where(t < early, 0, late)

    def columns_of(share, j):
        if aligned:
            return cot_ref.at[:, pl.ds(pl.multiple_of((share * own + j) * width, 128), width)]
        return cot_ref.at[share * own + j]

    def cot_copy(i):
        to = (dp - 1 - i // own + n) % n
        return send(columns_of(to, i % own), cot_in.at[i], x_send.at[i], x_recv.at[i], {"dp": to})

    def ids_copy(k):
        return send(
            ids_ref, ids_in.at[k - 1], i_send.at[k - 1, 0], i_recv.at[k - 1, 0], {"dp": (dp - k + n) % n}
        )

    def weights_copy(k):
        return send(
            weights_ref, weights_in.at[k - 1], i_send.at[k - 1, 1], i_recv.at[k - 1, 1], {"dp": (dp - k + n) % n}
        )

    def product_copy(k):
        return send(
            product.at[0], product.at[k], p_send.at[k - 1], p_recv.at[k - 1], {"dp": (dp - k + n) % n}
        )

    def up_copy(i):
        return send(up_out.at[i], up_in.at[i], u_send.at[i], u_recv.at[i], {"dp": (dp + 1 + i) % n})

    def pick(k, ids_row, weight_row):
        shape = (tokens, tokens)
        first = lax.broadcasted_iota(jnp.int32, shape, 0)
        second = lax.broadcasted_iota(jnp.int32, shape, 1)
        names = lax.broadcasted_iota(jnp.int32, (-(-experts // 16) * 16, tokens), 0) == ids_row
        before = jnp.where(first < second, 1.0, 0.0).astype(jnp.bfloat16)
        earlier = jnp.dot(
            jnp.where(names, 1.0, 0.0).astype(jnp.bfloat16), before, preferred_element_type=jnp.float32
        )
        position = jnp.sum(jnp.where(names, earlier, 0.0), axis=0, keepdims=True).astype(jnp.int32)
        target = ids_row * cap + position
        chosen = lax.broadcasted_iota(jnp.int32, (experts * cap, tokens), 0) == target
        picker[k] = jnp.where(chosen, 1.0, 0.0).astype(jnp.bfloat16)
        scale[k] = jnp.sum(jnp.where(chosen, weight_row, 0.0), axis=1, keepdims=True)

    def place(q, k, columns):
        picked = jnp.dot(picker[k], columns, preferred_element_type=jnp.float32)
        rows = (picked * scale[k]).astype(jnp.bfloat16).reshape(experts, cap, width)
        sendbuf[q] = rows
        routed[q, e, lane] = sendbuf[q, e]

    def build(t):
        q = chunk_at(t)

        @pl.when(q < own)
        def _():
            place(q, 0, columns_of(dp, q)[...])

        @pl.when(q >= own)
        def _():
            cot_copy(q - own).wait_recv()
            place(q, q // own, cot_in[q - own])

    def from_source(q, source):
        at = routed.at[q, source, lane]
        return send(at, at, y_send.at[q], y_recv.at[q], {"expert": across})

    def to_expert(t):
        q = chunk_at(t)
        for k in range(1, experts):
            there = (e + k) % experts
            send(
                sendbuf.at[q, there],
                routed.at[q, e, lane],
                z_send.at[q],
                z_recv.at[q],
                {"expert": there * SPLIT + lane},
            ).start()
        from_source(q, e).start()

    def over_y(q):
        at = routed.at[q, :, lane]
        return send(at, at, y_send.at[q], y_recv.at[q], {"expert": across})

    def over_core(q, turn):
        at = routed.at[q, :, lane if turn == 0 else lane_across]
        return send(at, at, c_send.at[q, turn], c_recv.at[q, turn], {"expert": beside})

    def all_but_one(ref_at, sem):
        pltpu.make_async_copy(ref_at, ref_at, sem).wait()

    loads[4].wait()
    loads[5].wait()
    pick(0, ids_ref[...], weights_ref[...])
    loads[0].wait()
    for j in range(early):
        place(j, 0, columns_of(dp, j)[...])
    pl.semaphore_wait(barrier, experts - 1 + 2 + n - 1)
    for k in range(1, n):
        ids_copy(k).start()
        weights_copy(k).start()

    @pl.loop(0, away)
    def _(i):
        cot_copy(i).start()

    for j in range(early):
        to_expert(j)

    rows_all = gate_ref.shape[0]
    piece = rows_all // 8
    loads[1].wait()
    loads[2].wait()

    @pl.loop(0, 8)
    def _(i):
        at = pl.ds(pl.multiple_of(i * piece, 16), piece)
        gate = gate_ref[at, :].astype(jnp.float32)
        up = up_ref[at, :].astype(jnp.float32)
        sig = jax.nn.sigmoid(gate)
        act = gate * sig
        active[at, :] = act
        slope[at, :] = up * sig * (1.0 + gate * (1.0 - sig))
        product[0, at, :] = (act * up).astype(jnp.bfloat16)
        for k in range(n):
            upstream[k, at, :] = jnp.zeros_like(act)

    for k in range(1, n):
        ids_copy(k).wait_recv()
        weights_copy(k).wait_recv()
        pick(k, ids_in[k - 1], weights_in[k - 1])
    for t in range(early, ahead):
        build(t)
    for t in range(early, ahead - 1):
        to_expert(t)
    for k in range(1, n):
        product_copy(k).start()
    loads[3].wait()

    def gradient(j):
        total = jnp.zeros((width, product.shape[2]), jnp.float32)
        for k in range(n):
            rows = routed[k * own + j].reshape(rows_all, width)
            total = total + lax.dot_general(
                rows, product[k], (((0,), (0,)), ((), ())), preferred_element_type=jnp.float32
            )
        wgrad_ref[j] = total.astype(jnp.bfloat16)

    @pl.loop(0, chunks + LAG + 1)
    def _(t):
        @pl.when(t + ahead < chunks)
        def _():
            build(t + ahead)

        @pl.when(t + ahead - 1 < chunks)
        def _():
            to_expert(t + ahead - 1)

        @pl.when(t < chunks)
        def _():
            q = chunk_at(t)
            all_but_one(routed.at[q, pl.ds(0, experts - 1), 0], z_recv.at[q])
            for k in range(1, experts):
                from_source(q, (e + k) % experts).start()
            over_core(q, 0).start()

        @pl.when((t >= LAG) & (t < chunks + LAG))
        def _():
            q = chunk_at(t - LAG)
            over_y(q).wait_recv()
            over_core(q, 1).start()

        @pl.when(t >= LAG + 1)
        def _():
            turn = t - LAG - 1
            q = chunk_at(turn)
            k, j = q // own, q % own
            over_core(q, 0).wait_recv()
            over_core(q, 1).wait_recv()
            rows = routed[q].reshape(rows_all, width)
            upstream[k] += jnp.dot(rows, down_ref[j], preferred_element_type=jnp.float32)

            @pl.when((k >= 1) & (j == own - 1))
            def _():
                up_out[k - 1] = upstream[k].astype(jnp.bfloat16)

            @pl.when(turn == early + away)
            def _():
                for i in range(1, n):
                    product_copy(i).wait_recv()
                for i in range(early):
                    gradient(i)

            @pl.when(turn >= early + away)
            def _():
                gradient(j)

            @pl.when((k >= 1) & (j == own - 1))
            def _():
                up_copy(k - 1).start()

    for k in range(1, n):
        up_copy(k - 1).wait_recv()

    @pl.loop(0, 8)
    def _(i):
        at = pl.ds(pl.multiple_of(i * piece, 16), piece)
        total = upstream[0, at, :]
        for k in range(1, n):
            total = total + up_in[k - 1, at, :].astype(jnp.float32)
        ggrad_ref[at, :] = (total * slope[at, :]).astype(jnp.bfloat16)
        ugrad_ref[at, :] = (total * active[at, :]).astype(jnp.bfloat16)

    @pl.loop(0, chunks)
    def _(q):
        all_but_one(sendbuf.at[q, pl.ds(0, experts - 1)], z_send.at[q])
        over_y(q).wait_send()
        over_core(q, 0).wait_send()
        over_core(q, 1).wait_send()

    @pl.loop(0, away)
    def _(i):
        cot_copy(i).wait_send()

    for k in range(1, n):
        ids_copy(k).wait_send()
        weights_copy(k).wait_send()
        product_copy(k).wait_send()
        up_copy(k - 1).wait_send()


def chunk_width(depth):
    for width in (256, 128):
        if depth % width == 0:
            return width, True
    return depth, False


def per_device(cotangent, expert_ids, route_weights, gate_pre, up_pre, down_weight):
    n = lax.axis_size("dp")
    devices = lax.axis_size("expert")
    experts = devices // SPLIT
    rows, hidden = gate_pre.shape
    capacity = rows // devices
    cap = -(-capacity // 16) * 16
    depth = down_weight.shape[0]
    width, aligned = chunk_width(depth)
    own = depth // width
    chunks = n * own
    away = chunks - own
    if not aligned:
        cotangent = cotangent.reshape(-1, chunks, width).swapaxes(0, 1)

    def widen(a):
        if cap == capacity:
            return a
        a = a.reshape(devices, capacity, hidden)
        return jnp.pad(a, ((0, 0), (0, cap - capacity), (0, 0))).reshape(devices * cap, hidden)

    def narrow(a):
        if cap == capacity:
            return a
        return a.reshape(devices, cap, hidden)[:, :capacity].reshape(rows, hidden)

    padded = devices * cap
    tokens = expert_ids.shape[0]
    half, full = jnp.bfloat16, jnp.float32
    vmem = pl.BlockSpec(memory_space=pltpu.VMEM)
    anywhere = pl.BlockSpec(memory_space=pltpu.HBM)
    dma = pltpu.SemaphoreType.DMA
    weight_grad, gate_grad, up_grad = pl.pallas_call(
        functools.partial(kernel, (n, experts, cap, chunks, width, aligned)),
        out_shape=(
            pltpu.VMEM((own, width, hidden), half),
            pltpu.VMEM((padded, hidden), half),
            pltpu.VMEM((padded, hidden), half),
        ),
        in_specs=[anywhere] * 6,
        out_specs=(vmem, vmem, vmem),
        scratch_shapes=[
            pltpu.VMEM(cotangent.shape, half),
            pltpu.VMEM((1, tokens), jnp.int32),
            pltpu.VMEM((1, tokens), full),
            pltpu.VMEM((padded, hidden), half),
            pltpu.VMEM((padded, hidden), half),
            pltpu.VMEM((own, width, hidden), half),
            dma((6,)),
            pltpu.VMEM((chunks, experts, cap, width), half),
            pltpu.VMEM((chunks, experts, SPLIT, cap, width), half),
            pltpu.VMEM((away, tokens, width), half),
            pltpu.VMEM((n - 1, 1, tokens), jnp.int32),
            pltpu.VMEM((n - 1, 1, tokens), full),
            pltpu.VMEM((n - 1, padded, hidden), half),
            pltpu.VMEM((n - 1, padded, hidden), half),
            pltpu.VMEM((n, padded, hidden), full),
            pltpu.VMEM((padded, hidden), full),
            pltpu.VMEM((padded, hidden), full),
            pltpu.VMEM((n, padded, hidden), half),
            pltpu.VMEM((n, experts * cap, tokens), half),
            pltpu.VMEM((n, experts * cap, 1), full),
            dma((chunks,)),
            dma((chunks,)),
            dma((chunks,)),
            dma((chunks,)),
            dma((chunks, 2)),
            dma((chunks, 2)),
            dma((away,)),
            dma((away,)),
            dma((n - 1, 2)),
            dma((n - 1, 2)),
            dma((n - 1,)),
            dma((n - 1,)),
            dma((n - 1,)),
            dma((n - 1,)),
        ],
        compiler_params=pltpu.CompilerParams(collective_id=0, has_side_effects=True),
    )(
        cotangent,
        expert_ids.reshape(1, -1),
        route_weights.reshape(1, -1),
        widen(gate_pre),
        widen(up_pre),
        down_weight.reshape(own, width, hidden),
    )
    return weight_grad.reshape(depth, hidden), narrow(gate_grad), narrow(up_grad)


def solution(mesh):
    placed = (
        P(("dp", "expert"), None),
        P(("dp", "expert"), None),
        P(("dp", "expert"), None),
        P("dp", "expert"),
        P("dp", "expert"),
        P("dp", "expert"),
    )
    return jax.shard_map(
        per_device,
        mesh=mesh,
        in_specs=placed,
        out_specs=(P("dp", "expert"), P("dp", "expert"), P("dp", "expert")),
        check_vma=False,
    )
```

```python
import functools

import jax
import jax.numpy as jnp
from jax import lax
from jax.experimental import pallas as pl
from jax.experimental.pallas import tpu as pltpu
from jax.sharding import PartitionSpec as P

SPLIT = 4
EARLY = 2
BUILD = 3
LAG = 2


def kernel(
    sizes,
    cot_hbm,
    ids_hbm,
    weights_hbm,
    gate_hbm,
    up_hbm,
    down_hbm,
    wgrad_ref,
    ggrad_ref,
    ugrad_ref,
    cot_ref,
    ids_ref,
    weights_ref,
    gate_ref,
    up_ref,
    down_ref,
    load,
    sendbuf,
    routed,
    cot_in,
    ids_in,
    weights_in,
    up_out,
    up_in,
    upstream,
    slope,
    active,
    product,
    picker,
    scale,
    z_send,
    z_recv,
    y_send,
    y_recv,
    c_send,
    c_recv,
    x_send,
    x_recv,
    i_send,
    i_recv,
    p_send,
    p_recv,
    u_send,
    u_recv,
):
    n, experts, cap, chunks, width, aligned = sizes
    own = chunks // n
    away = chunks - own
    early = min(EARLY, own - 1)
    ahead = min(BUILD, chunks)
    tokens = ids_ref.shape[1]
    dp = lax.axis_index("dp")
    me = lax.axis_index("expert")
    e, lane = me // SPLIT, me % SPLIT
    across = me - lane + (lane + 2) % SPLIT
    beside = me - lane + (lane // 2) * 2 + (lane + 1) % 2
    lane_across = (lane + 2) % SPLIT

    loads = [
        pltpu.make_async_copy(source, to, load.at[i])
        for i, (source, to) in enumerate(
            (
                (cot_hbm, cot_ref),
                (gate_hbm, gate_ref),
                (up_hbm, up_ref),
                (down_hbm, down_ref),
                (ids_hbm, ids_ref),
                (weights_hbm, weights_ref),
            )
        )
    ]
    for i in (4, 5, 0, 1, 2, 3):
        loads[i].start()

    barrier = pltpu.get_barrier_semaphore()

    def greet(target):
        pl.semaphore_signal(
            barrier, inc=1, device_id=target, device_id_type=pl.DeviceIdType.MESH
        )

    for k in range(1, experts):
        greet({"expert": (e + k) % experts * SPLIT + lane})
    greet({"expert": across})
    greet({"expert": beside})
    for k in range(1, n):
        greet({"dp": (dp + k) % n})

    def send(source, to, sent, arrived, device):
        return pltpu.make_async_remote_copy(
            src_ref=source,
            dst_ref=to,
            send_sem=sent,
            recv_sem=arrived,
            device_id=device,
            device_id_type=pl.DeviceIdType.MESH,
        )

    def chunk_at(t):
        late = jnp.where(t < early + away, own - early, -away)
        return t + jnp.where(t < early, 0, late)

    def columns_of(share, j):
        if aligned:
            return cot_ref.at[:, pl.ds(pl.multiple_of((share * own + j) * width, 128), width)]
        return cot_ref.at[share * own + j]

    def cot_copy(i):
        to = (dp - 1 - i // own + n) % n
        return send(columns_of(to, i % own), cot_in.at[i], x_send.at[i], x_recv.at[i], {"dp": to})

    def ids_copy(k):
        return send(
            ids_ref, ids_in.at[k - 1], i_send.at[k - 1, 0], i_recv.at[k - 1, 0], {"dp": (dp - k + n) % n}
        )

    def weights_copy(k):
        return send(
            weights_ref, weights_in.at[k - 1], i_send.at[k - 1, 1], i_recv.at[k - 1, 1], {"dp": (dp - k + n) % n}
        )

    def product_copy(k):
        return send(
            product.at[0], product.at[k], p_send.at[k - 1], p_recv.at[k - 1], {"dp": (dp - k + n) % n}
        )

    def up_copy(i):
        return send(up_out.at[i], up_in.at[i], u_send.at[i], u_recv.at[i], {"dp": (dp + 1 + i) % n})

    def pick(k, ids_row, weight_row):
        shape = (tokens, tokens)
        first = lax.broadcasted_iota(jnp.int32, shape, 0)
        second = lax.broadcasted_iota(jnp.int32, shape, 1)
        names = lax.broadcasted_iota(jnp.int32, (-(-experts // 16) * 16, tokens), 0) == ids_row
        before = jnp.where(first < second, 1.0, 0.0).astype(jnp.bfloat16)
        earlier = jnp.dot(
            jnp.where(names, 1.0, 0.0).astype(jnp.bfloat16), before, preferred_element_type=jnp.float32
        )
        position = jnp.sum(jnp.where(names, earlier, 0.0), axis=0, keepdims=True).astype(jnp.int32)
        target = ids_row * cap + position
        chosen = lax.broadcasted_iota(jnp.int32, (experts * cap, tokens), 0) == target
        picker[k] = jnp.where(chosen, 1.0, 0.0).astype(jnp.bfloat16)
        scale[k] = jnp.sum(jnp.where(chosen, weight_row, 0.0), axis=1, keepdims=True)

    def place(q, k, columns):
        picked = jnp.dot(picker[k], columns, preferred_element_type=jnp.float32)
        rows = (picked * scale[k]).astype(jnp.bfloat16).reshape(experts, cap, width)
        sendbuf[q] = rows
        routed[q, e, lane] = sendbuf[q, e]

    def build(t):
        q = chunk_at(t)

        @pl.when(q < own)
        def _():
            place(q, 0, columns_of(dp, q)[...])

        @pl.when(q >= own)
        def _():
            cot_copy(q - own).wait_recv()
            place(q, q // own, cot_in[q - own])

    def from_source(q, source):
        at = routed.at[q, source, lane]
        return send(at, at, y_send.at[q], y_recv.at[q], {"expert": across})

    def to_expert(t):
        q = chunk_at(t)
        for k in range(1, experts):
            there = (e + k) % experts
            send(
                sendbuf.at[q, there],
                routed.at[q, e, lane],
                z_send.at[q],
                z_recv.at[q],
                {"expert": there * SPLIT + lane},
            ).start()
        from_source(q, e).start()

    def over_y(q):
        at = routed.at[q, :, lane]
        return send(at, at, y_send.at[q], y_recv.at[q], {"expert": across})

    def over_core(q, turn):
        at = routed.at[q, :, lane if turn == 0 else lane_across]
        return send(at, at, c_send.at[q, turn], c_recv.at[q, turn], {"expert": beside})

    def all_but_one(ref_at, sem):
        pltpu.make_async_copy(ref_at, ref_at, sem).wait()

    loads[4].wait()
    loads[5].wait()
    pick(0, ids_ref[...], weights_ref[...])
    loads[0].wait()
    for j in range(early):
        place(j, 0, columns_of(dp, j)[...])
    pl.semaphore_wait(barrier, experts - 1 + 2 + n - 1)
    for k in range(1, n):
        ids_copy(k).start()
        weights_copy(k).start()

    @pl.loop(0, away)
    def _(i):
        cot_copy(i).start()

    for j in range(early):
        to_expert(j)

    rows_all = gate_ref.shape[0]
    piece = rows_all // 8
    loads[1].wait()
    loads[2].wait()

    @pl.loop(0, 8)
    def _(i):
        at = pl.ds(pl.multiple_of(i * piece, 16), piece)
        gate = gate_ref[at, :].astype(jnp.float32)
        up = up_ref[at, :].astype(jnp.float32)
        sig = jax.nn.sigmoid(gate)
        act = gate * sig
        active[at, :] = act
        slope[at, :] = up * sig * (1.0 + gate * (1.0 - sig))
        product[0, at, :] = (act * up).astype(jnp.bfloat16)
        for k in range(n):
            upstream[k, at, :] = jnp.zeros_like(act)

    for k in range(1, n):
        ids_copy(k).wait_recv()
        weights_copy(k).wait_recv()
        pick(k, ids_in[k - 1], weights_in[k - 1])
    for t in range(early, ahead):
        build(t)
    for t in range(early, ahead - 1):
        to_expert(t)
    for k in range(1, n):
        product_copy(k).start()
    loads[3].wait()

    def gradient(j):
        total = jnp.zeros((width, product.shape[2]), jnp.float32)
        for k in range(n):
            rows = routed[k * own + j].reshape(rows_all, width)
            total = total + lax.dot_general(
                rows, product[k], (((0,), (0,)), ((), ())), preferred_element_type=jnp.float32
            )
        wgrad_ref[j] = total.astype(jnp.bfloat16)

    @pl.loop(0, chunks + LAG + 1)
    def _(t):
        @pl.when(t + ahead < chunks)
        def _():
            build(t + ahead)

        @pl.when(t + ahead - 1 < chunks)
        def _():
            to_expert(t + ahead - 1)

        @pl.when(t < chunks)
        def _():
            q = chunk_at(t)
            all_but_one(routed.at[q, pl.ds(0, experts - 1), 0], z_recv.at[q])
            for k in range(1, experts):
                from_source(q, (e + k) % experts).start()
            over_core(q, 0).start()

        @pl.when((t >= LAG) & (t < chunks + LAG))
        def _():
            q = chunk_at(t - LAG)
            over_y(q).wait_recv()
            over_core(q, 1).start()

        @pl.when(t >= LAG + 1)
        def _():
            turn = t - LAG - 1
            q = chunk_at(turn)
            k, j = q // own, q % own
            over_core(q, 0).wait_recv()
            over_core(q, 1).wait_recv()
            rows = routed[q].reshape(rows_all, width)
            upstream[k] += jnp.dot(rows, down_ref[j], preferred_element_type=jnp.float32)

            @pl.when((k >= 1) & (j == own - 1))
            def _():
                up_out[k - 1] = upstream[k].astype(jnp.bfloat16)

            @pl.when(turn == early + away)
            def _():
                for i in range(1, n):
                    product_copy(i).wait_recv()
                for i in range(early):
                    gradient(i)

            @pl.when(turn >= early + away)
            def _():
                gradient(j)

            @pl.when((k >= 1) & (j == own - 1))
            def _():
                up_copy(k - 1).start()

    for k in range(1, n):
        up_copy(k - 1).wait_recv()

    @pl.loop(0, 8)
    def _(i):
        at = pl.ds(pl.multiple_of(i * piece, 16), piece)
        total = upstream[0, at, :]
        for k in range(1, n):
            total = total + up_in[k - 1, at, :].astype(jnp.float32)
        ggrad_ref[at, :] = (total * slope[at, :]).astype(jnp.bfloat16)
        ugrad_ref[at, :] = (total * active[at, :]).astype(jnp.bfloat16)

    @pl.loop(0, chunks)
    def _(q):
        all_but_one(sendbuf.at[q, pl.ds(0, experts - 1)], z_send.at[q])
        over_y(q).wait_send()
        over_core(q, 0).wait_send()
        over_core(q, 1).wait_send()

    @pl.loop(0, away)
    def _(i):
        cot_copy(i).wait_send()

    for k in range(1, n):
        ids_copy(k).wait_send()
        weights_copy(k).wait_send()
        product_copy(k).wait_send()
        up_copy(k - 1).wait_send()


def chunk_width(depth):
    for width in (256, 128):
        if depth % width == 0:
            return width, True
    return depth, False


def per_device(cotangent, expert_ids, route_weights, gate_pre, up_pre, down_weight):
    n = lax.axis_size("dp")
    devices = lax.axis_size("expert")
    experts = devices // SPLIT
    rows, hidden = gate_pre.shape
    capacity = rows // devices
    cap = -(-capacity // 16) * 16
    depth = down_weight.shape[0]
    width, aligned = chunk_width(depth)
    own = depth // width
    chunks = n * own
    away = chunks - own
    if not aligned:
        cotangent = cotangent.reshape(-1, chunks, width).swapaxes(0, 1)

    def widen(a):
        if cap == capacity:
            return a
        a = a.reshape(devices, capacity, hidden)
        return jnp.pad(a, ((0, 0), (0, cap - capacity), (0, 0))).reshape(devices * cap, hidden)

    def narrow(a):
        if cap == capacity:
            return a
        return a.reshape(devices, cap, hidden)[:, :capacity].reshape(rows, hidden)

    padded = devices * cap
    tokens = expert_ids.shape[0]
    half, full = jnp.bfloat16, jnp.float32
    vmem = pl.BlockSpec(memory_space=pltpu.VMEM)
    anywhere = pl.BlockSpec(memory_space=pltpu.HBM)
    dma = pltpu.SemaphoreType.DMA
    weight_grad, gate_grad, up_grad = pl.pallas_call(
        functools.partial(kernel, (n, experts, cap, chunks, width, aligned)),
        out_shape=(
            pltpu.VMEM((own, width, hidden), half),
            pltpu.VMEM((padded, hidden), half),
            pltpu.VMEM((padded, hidden), half),
        ),
        in_specs=[anywhere] * 6,
        out_specs=(vmem, vmem, vmem),
        scratch_shapes=[
            pltpu.VMEM(cotangent.shape, half),
            pltpu.VMEM((1, tokens), jnp.int32),
            pltpu.VMEM((1, tokens), full),
            pltpu.VMEM((padded, hidden), half),
            pltpu.VMEM((padded, hidden), half),
            pltpu.VMEM((own, width, hidden), half),
            dma((6,)),
            pltpu.VMEM((chunks, experts, cap, width), half),
            pltpu.VMEM((chunks, experts, SPLIT, cap, width), half),
            pltpu.VMEM((away, tokens, width), half),
            pltpu.VMEM((n - 1, 1, tokens), jnp.int32),
            pltpu.VMEM((n - 1, 1, tokens), full),
            pltpu.VMEM((n - 1, padded, hidden), half),
            pltpu.VMEM((n - 1, padded, hidden), half),
            pltpu.VMEM((n, padded, hidden), full),
            pltpu.VMEM((padded, hidden), full),
            pltpu.VMEM((padded, hidden), full),
            pltpu.VMEM((n, padded, hidden), half),
            pltpu.VMEM((n, experts * cap, tokens), half),
            pltpu.VMEM((n, experts * cap, 1), full),
            dma((chunks,)),
            dma((chunks,)),
            dma((chunks,)),
            dma((chunks,)),
            dma((chunks, 2)),
            dma((chunks, 2)),
            dma((away,)),
            dma((away,)),
            dma((n - 1, 2)),
            dma((n - 1, 2)),
            dma((n - 1,)),
            dma((n - 1,)),
            dma((n - 1,)),
            dma((n - 1,)),
        ],
        compiler_params=pltpu.CompilerParams(collective_id=0, has_side_effects=True),
    )(
        cotangent,
        expert_ids.reshape(1, -1),
        route_weights.reshape(1, -1),
        widen(gate_pre),
        widen(up_pre),
        down_weight.reshape(own, width, hidden),
    )
    return weight_grad.reshape(depth, hidden), narrow(gate_grad), narrow(up_grad)


def solution(mesh):
    placed = (
        P(("dp", "expert"), None),
        P(("dp", "expert"), None),
        P(("dp", "expert"), None),
        P("dp", "expert"),
        P("dp", "expert"),
        P("dp", "expert"),
    )
    return jax.shard_map(
        per_device,
        mesh=mesh,
        in_specs=placed,
        out_specs=(P("dp", "expert"), P("dp", "expert"), P("dp", "expert")),
        check_vma=False,
    )
```
